32 devices in a mesh: seq: 8 (over z, x), img: 2 (over y), fsdp: 2 (over core).
Axes of the slice: x: 2, y: 2, z: 4, core: 2. Of those that a mesh axis runs over, the one named last changes fastest.
Arguments:
- vision_feats: bfloat16 [2, 2304, 1024], P('img', ('seq', 'fsdp')), may hold values from -6 to 6
- ln_gain: float32 [1024], replicated, may hold values from 0.5 to 1.5
- ln_bias: float32 [1024], replicated, may hold values from -3 to 3
- w_in: bfloat16 [1024, 4096], P('fsdp', 'seq'), may hold values from -0.1875 to 0.1875
- b_in: float32 [4096], P('seq'), may hold values from -3 to 3
- w_out: bfloat16 [4096, 4096], P('seq', 'fsdp'), may hold values from -0.09375 to 0.09375
- lm_grad: bfloat16 [2, 4096, 4096], P('img', 'seq', 'fsdp'), may hold values from -0.079589844 to 0.079589844
- image_counts: int32 [2, 2], P('img'), may hold values from 1 to 3, as said below
- token_pos: int32 [2, 2304], P('img'), may hold values from 0 to 2047, as said below
Outputs:
- w_in_grad: float32 [1024, 4096], P(('img', 'fsdp'), 'seq')
- b_in_grad: float32 [4096], replicated
- w_out_grad: float32 [4096, 4096], P(('seq', 'img'), 'fsdp')
- b_out_grad: float32 [4096], replicated
- ln_gain_grad: float32 [1024], replicated
- ln_bias_grad: float32 [1024], replicated
The draws below stay inside these ranges and needn't reach their ends.
Inputs may be any that keep to these rules, and one draw needn't show every extreme that they name: `image_counts`: in each group the 2 samples hold 4 images together, each sample one or more. `token_pos`: each image's 576 tokens take consecutive positions of its sample's sequence in order; a sample's images come in order without intersection, and images are numbered sample by sample as image_counts gives.
All inputs are finite; a program needn't handle non-finite values.
Results may differ from the reference program's by a relative error of at most 0.0047.
Values may be sent and summed in bfloat16 or wider, within the bound.
A program may use at most 128 MiB of HBM per device.

```python
import jax
import jax.numpy as jnp
from jax import lax

D = 4096
DV = 1024
HID = 4096
PATCH = 576
IMGS = 4
LEN = 2048
IMG_ROWS = 2304
POS = 4096
GROUPS = 2


def image_layout(key):
    base_key = jax.random.fold_in(key, 311)
    count_key, place_key = jax.random.split(base_key)
    first_count = 1 + jax.random.randint(count_key, (GROUPS,), 0, 3)
    counts = jnp.stack([first_count, IMGS - first_count], axis=1).astype(jnp.int32)
    text_room = LEN - counts * PATCH
    marks = jax.random.randint(place_key, (GROUPS, 2, 3), 0, 1 + text_room[:, :, None])
    marks = jnp.sort(marks, axis=2).astype(jnp.int32)
    pieces = []
    for image_index in range(IMGS):
        in_second = image_index >= first_count
        sample = in_second.astype(jnp.int32)
        slot_index = jnp.where(in_second, image_index - first_count, image_index).astype(jnp.int32)
        mark_row = jnp.take_along_axis(marks, sample[:, None, None], axis=1)[:, 0, :]
        begin_pos = jnp.take_along_axis(mark_row, slot_index[:, None], axis=1)[:, 0] + slot_index * PATCH
        pieces.append(begin_pos[:, None] + jnp.arange(PATCH, dtype=jnp.int32)[None, :])
    positions = jnp.concatenate(pieces, axis=1).astype(jnp.int32)
    return (counts, positions)


def draw_image_counts(key, part):
    counts, positions = image_layout(key)
    return counts


def draw_token_pos(key, part):
    counts, positions = image_layout(key)
    return positions


def shard_levels(key, shape, cuts, low, top_value):
    def one(position, parts):
        draws = jax.random.uniform(jax.random.fold_in(jax.random.fold_in(key, 6), position), (parts,), jnp.float32, low / len(cuts), top_value / len(cuts))
        return jnp.repeat(jnp.exp(draws), shape[position] // parts).reshape((-1,) + (1,) * (len(shape) - position - 1))

    loudness = one(*cuts[0])
    for cut in cuts[1:]:
        loudness = loudness * one(*cut)
    return loudness


def normal_values(stream_key, extent, deviation, limit, cuts=(), held_as=jnp.bfloat16):
    entries = jax.random.normal(stream_key, extent, jnp.float32) * deviation
    if len(cuts) > 0:
        entries = shard_levels(stream_key, extent, cuts, -0.22, 0.18) * entries
    return jnp.clip(entries, min=-limit, max=limit).astype(held_as)


def setup_inputs(seed: int = 0) -> dict:
    arg_keys = jax.random.split(jax.random.key(seed), 10)
    return {
        "vision_feats": normal_values(arg_keys[0], (GROUPS, IMG_ROWS, DV), 1.0, 6.0, ((0, 2), (1, 16))),
        "ln_gain": jnp.clip(1.0 + 0.1 * jax.random.normal(arg_keys[1], (DV,), jnp.float32), 0.5, 1.5),
        "ln_bias": normal_values(arg_keys[2], (DV,), 0.5, 3.0, (), jnp.float32),
        "w_in": normal_values(arg_keys[3], (DV, HID), DV ** -0.5, 0.1875, ((0, 2), (1, 8))),
        "b_in": normal_values(arg_keys[4], (HID,), 0.5, 3.0, ((0, 8),), jnp.float32),
        "w_out": normal_values(arg_keys[5], (HID, D), HID ** -0.5, 0.09375, ((0, 8), (1, 2))),
        "lm_grad": normal_values(arg_keys[6], (GROUPS, POS, D), 0.01, 0.079589844, ((0, 2), (1, 8), (2, 2))),
        "image_counts": draw_image_counts(jax.random.fold_in(arg_keys[9], 71), 0),
        "token_pos": draw_token_pos(jax.random.fold_in(arg_keys[9], 71), 0),
    }


def gelu_parts(preact):
    cumul = 0.5 * (1.0 + lax.erf(preact * 0.7071067811865476))
    density = jnp.exp(-0.5 * preact * preact) * 0.3989422804014327
    return (preact * cumul, cumul + preact * density)

def layer_norm(features, ln_gain, ln_bias):
    values = features.astype(jnp.float32)
    row_mean = lax.optimization_barrier(jnp.mean(values, axis=1, keepdims=True))
    centred = values - row_mean
    row_var = lax.optimization_barrier(jnp.mean(centred * centred, axis=1, keepdims=True))
    normed = centred * lax.rsqrt(row_var + 1e-05)
    return (normed, (normed * ln_gain + ln_bias).astype(jnp.bfloat16))

def absolute_positions(counts, positions):
    row_count = positions.shape[0]
    image_index = jnp.arange(row_count, dtype=jnp.int32) // PATCH
    bounds = jnp.cumsum(counts).astype(jnp.int32)
    sample = lax.optimization_barrier(jnp.sum((image_index[:, None] >= bounds[None, :]).astype(jnp.int32), axis=1))
    return (sample * LEN + positions).astype(jnp.int32)

def contract(left, right, left_dim, right_dim):
    return lax.dot_general(left, right, (((left_dim,), (right_dim,)), ((), ())), preferred_element_type=jnp.float32)

def reference(vision_feats, ln_gain, ln_bias, w_in, b_in, w_out, lm_grad, image_counts, token_pos):

    def one_group(totals, inputs):
        features, cotangent, counts, positions = inputs
        normed, normed_in = layer_norm(features, ln_gain, ln_bias)
        preact = jnp.dot(normed_in, w_in, preferred_element_type=jnp.float32) + b_in
        activ, slope = gelu_parts(preact)
        hidden = activ.astype(jnp.bfloat16)
        picked = cotangent[absolute_positions(counts, positions)]
        hidden_grad = contract(picked, w_out, 1, 1)
        preact_grad = (hidden_grad * slope).astype(jnp.bfloat16)
        normed_grad = contract(preact_grad, w_in, 1, 1)
        terms = (contract(normed_in, preact_grad, 0, 0), lax.optimization_barrier(jnp.sum(preact_grad, axis=0, dtype=jnp.float32)), contract(hidden, picked, 0, 0), lax.optimization_barrier(jnp.sum(picked, axis=0, dtype=jnp.float32)), lax.optimization_barrier(jnp.sum(normed_grad * normed, axis=0)), lax.optimization_barrier(jnp.sum(normed_grad, axis=0)))
        return (tuple((left + right for left, right in zip(totals, terms))), None)
    start_state = (jnp.zeros((DV, HID), jnp.float32), jnp.zeros((HID,), jnp.float32), jnp.zeros((HID, D), jnp.float32), jnp.zeros((D,), jnp.float32), jnp.zeros((DV,), jnp.float32), jnp.zeros((DV,), jnp.float32))
    totals, unused = lax.scan(one_group, start_state, (vision_feats, lm_grad, image_counts, token_pos))
    return (totals[0], totals[1], totals[2], totals[3], totals[4], totals[5])
```

```python
import jax
import jax.numpy as jnp
from jax import lax
from jax.sharding import PartitionSpec as P

PATCH = 576
CHUNKS = 2


def gelu_parts(preact):
    cumul = 0.5 * (1.0 + lax.erf(preact * 0.7071067811865476))
    density = jnp.exp(-0.5 * preact * preact) * 0.3989422804014327
    return (preact * cumul, cumul + preact * density)


def contract(left, right, left_dim, right_dim):
    return lax.dot_general(
        left, right, (((left_dim,), (right_dim,)), ((), ())), preferred_element_type=jnp.float32
    )


def shift(value, axis, amount):
    count = lax.axis_size(axis)
    return lax.ppermute(value, axis, [(i, (i + amount) % count) for i in range(count)])


def flip(value, bit):
    count = lax.axis_size("seq")
    return lax.ppermute(value, "seq", [(i, i ^ bit) for i in range(count)])


def pick(value, index, axis):
    return lax.dynamic_index_in_dim(value, index, axis=axis, keepdims=False)


def scatter_sum(value, axis):
    count = lax.axis_size(axis)
    index = lax.axis_index(axis)
    if count > 2:
        return lax.psum_scatter(value, axis, scatter_dimension=0, tiled=False)
    if count == 1:
        return value[0]
    sent = pick(value, 1 - index, 0).astype(jnp.bfloat16)
    return pick(value, index, 0) + shift(sent, axis, 1).astype(jnp.float32)


def sample_sum(value, stride, after):
    total, _ = lax.optimization_barrier((value[0], after))
    for k in range(1, value.shape[0]):
        moved = shift(value[k].astype(jnp.bfloat16), "seq", -k * stride)
        total = total + moved.astype(jnp.float32)
    return total


def per_device(vision_feats, ln_gain, ln_bias, w_in, b_in, w_out, lm_grad, image_counts, token_pos):
    seq_count = lax.axis_size("seq")
    seq_index = lax.axis_index("seq")
    img_count = lax.axis_size("img")
    fsdp_count = lax.axis_size("fsdp")
    fsdp_index = lax.axis_index("fsdp")
    lm_block = lm_grad[0]
    block_rows, half_width = lm_block.shape
    counts = image_counts[0]
    samples = counts.shape[0]
    stride = seq_count // samples
    sample_len = stride * block_rows
    own_sample = seq_index // stride
    positions = token_pos[0]
    row_count = positions.shape[0]
    images = row_count // PATCH
    starts = positions.reshape(images, PATCH)[:, 0]
    bounds = jnp.cumsum(counts)
    image_index = jnp.arange(images, dtype=jnp.int32)
    image_sample = jnp.sum((image_index[:, None] >= bounds[None, :]).astype(jnp.int32), axis=1)
    in_sample = image_sample == own_sample

    def lookup(place):
        offset = place[:, None] - starts[None, :]
        match = in_sample[None, :] & (offset >= 0) & (offset < PATCH)
        row = jnp.sum(jnp.where(match, offset + image_index[None, :] * PATCH, 0), axis=1)
        return row, jnp.any(match, axis=1)

    own_place = (seq_index % stride) * block_rows + jnp.arange(block_rows, dtype=jnp.int32)
    own_mask = lookup(own_place)[1].astype(jnp.bfloat16)
    out_bias_half = jnp.dot(own_mask[None, :], lm_block, preferred_element_type=jnp.float32)[0]
    out_bias_whole = lax.dynamic_update_slice_in_dim(
        jnp.zeros((half_width * fsdp_count,), jnp.float32),
        out_bias_half,
        fsdp_index * half_width,
        0,
    )

    feats = lax.all_gather(vision_feats[0], ("seq", "fsdp"), axis=0, tiled=True)

    in_blocks = [w_in] + [shift(w_in, "seq", k * stride) for k in range(1, samples)]
    in_bias = jnp.concatenate([b_in] + [shift(b_in, "seq", k * stride) for k in range(1, samples)])
    w_in_half = jnp.concatenate(in_blocks, axis=1)
    w_in_full = lax.all_gather(w_in_half, "fsdp", axis=0, tiled=True)
    w_out_later, _ = lax.optimization_barrier((w_out, w_in_half))
    w_out_full = jnp.concatenate(
        [w_out] + [shift(w_out_later, "seq", k * stride) for k in range(1, samples)], axis=0
    )
    hid = in_bias.shape[0]
    block_hid = hid // samples

    groups = [[s * stride + i for i in range(stride)] for s in range(samples)]
    width = half_width // CHUNKS
    slices = [lm_block[:, c * width : (c + 1) * width] for c in range(CHUNKS)]
    crossed = stride == 4
    if crossed:
        pieces = []
        for piece in slices:
            far = flip(piece, 2)
            near = flip(piece, 1)
            pieces.append(jnp.concatenate([piece, near, far, flip(far, 1)], axis=0))
    else:
        pieces = [
            lax.all_gather(piece, "seq", axis=0, tiled=True, axis_index_groups=groups)
            for piece in slices
        ]
    b_out_grad = lax.psum(out_bias_whole, ("seq", "img", "fsdp"))
    feats, b_out_grad = lax.optimization_barrier((feats, b_out_grad))

    part_len = sample_len // fsdp_count
    place = fsdp_index * part_len + jnp.arange(part_len, dtype=jnp.int32)
    if crossed:
        block = place // block_rows
        place = (block ^ (seq_index % stride)) * block_rows + place % block_rows
    row, mask = lookup(place)
    values = feats.at[row].get(mode="promise_in_bounds").astype(jnp.float32)
    row_mean = jnp.mean(values, axis=1, keepdims=True)
    centred = values - row_mean
    row_var = jnp.mean(centred * centred, axis=1, keepdims=True)
    normed = centred * lax.rsqrt(row_var + 1e-05)
    normed_in = (normed * ln_gain + ln_bias).astype(jnp.bfloat16)
    preact = jnp.dot(normed_in, w_in_full, preferred_element_type=jnp.float32) + in_bias
    activ, slope = gelu_parts(preact)
    hidden = jnp.where(mask[:, None], activ, 0.0).astype(jnp.bfloat16)
    slope = jnp.where(mask[:, None], slope, 0.0)
    if fsdp_count == 2:
        other = shift(hidden, "fsdp", 1)
        first = fsdp_index == 0
        hidden_full = jnp.concatenate(
            [jnp.where(first, hidden, other), jnp.where(first, other, hidden)], axis=0
        )
    else:
        hidden_full = lax.all_gather(hidden, "fsdp", axis=0, tiled=True)

    w_out_grads = []
    hidden_part = 0.0
    hidden_full, pieces[0] = lax.optimization_barrier((hidden_full, pieces[0]))
    for c in range(CHUNKS):
        piece = pieces[c]
        part = contract(hidden_full, piece, 0, 0)
        part = part.reshape(samples, img_count, block_hid // img_count, width)
        part = scatter_sum(part.transpose(1, 0, 2, 3), "img")
        w_out_grads.append(part)
        hidden_part = hidden_part + contract(
            piece, w_out_full[:, c * width : (c + 1) * width], 1, 1
        )

    hidden_grad = scatter_sum(hidden_part.reshape(fsdp_count, part_len, hid), "fsdp")
    preact_grad = (hidden_grad * slope).astype(jnp.bfloat16)
    in_part = contract(normed_in, preact_grad, 0, 0)
    in_part = in_part.reshape(img_count, fsdp_count, -1, samples, block_hid)
    in_part = scatter_sum(in_part.transpose(1, 0, 2, 3, 4), "fsdp")
    in_part = scatter_sum(in_part, "img")

    b_in_part = jnp.sum(preact_grad, axis=0, dtype=jnp.float32)
    normed_grad = contract(preact_grad, w_in_full, 1, 1)
    gain_part = jnp.sum(normed_grad * normed, axis=0)
    bias_part = jnp.sum(normed_grad, axis=0)
    hidden_bias = jnp.zeros((seq_count, block_hid), jnp.float32)
    for k in range(samples):
        owner = (seq_index - k * stride + seq_count) % seq_count
        hidden_bias = lax.dynamic_update_slice(
            hidden_bias, b_in_part[None, k * block_hid : (k + 1) * block_hid], (owner, 0)
        )
    gain_grad, bias_grad, b_in_grad = lax.psum(
        (gain_part, bias_part, hidden_bias.reshape(-1)), ("seq", "img", "fsdp")
    )
    w_in_grad = sample_sum(in_part.transpose(1, 0, 2), stride, gain_grad)
    w_out_grad = jnp.concatenate(
        [sample_sum(part, stride, gain_grad) for part in w_out_grads], axis=1
    )
    return (w_in_grad, b_in_grad, w_out_grad, b_out_grad, gain_grad, bias_grad)


def solution(mesh):
    return jax.shard_map(
        per_device,
        mesh=mesh,
        in_specs=(
            P("img", ("seq", "fsdp"), None),
            P(),
            P(),
            P("fsdp", "seq"),
            P("seq"),
            P("seq", "fsdp"),
            P("img", "seq", "fsdp"),
            P("img", None),
            P("img", None),
        ),
        out_specs=(
            P(("img", "fsdp"), "seq"),
            P(),
            P(("seq", "img"), "fsdp"),
            P(),
            P(),
            P(),
        ),
        check_vma=False,
    )
```
